16 devices in a mesh: dp: 4 (over y, z, core), tp: 4 (over x).
Axes of the slice: x: 4, y: 2, z: 1, core: 2. Of those that a mesh axis runs over, the one named last changes fastest.
The devices are a block of a 4x4x8 slice.
Arguments:
- x: bfloat16 [4, 2048, 2560], P('dp', 'tp'), parts along dimension 0
- dy: bfloat16 [4, 2048, 2560], P('dp', 'tp'), parts along dimension 0
- wq: bfloat16 [2560, 4096], P(None, 'tp')
- wk: bfloat16 [2560, 1024], P(None, 'tp')
- wv: bfloat16 [2560, 1024], P(None, 'tp')
- wo: bfloat16 [4096, 2560], P('tp')
- w_gate: bfloat16 [2560, 9728], P(None, 'tp')
- w_up: bfloat16 [2560, 9728], P(None, 'tp')
- w_down: bfloat16 [9728, 2560], P('tp')
Outputs:
- output 1: bfloat16 [4, 2048, 2560], P('dp', 'tp'), parts along dimension 0
- output 2: bfloat16 [10240, 4096], P('dp', 'tp'), parts along dimension 0
- output 3: bfloat16 [10240, 1024], P('dp', 'tp'), parts along dimension 0
- output 4: bfloat16 [10240, 1024], P('dp', 'tp'), parts along dimension 0
- output 5: bfloat16 [16384, 2560], P(('dp', 'tp')), parts along dimension 0
- output 6: bfloat16 [10240, 9728], P('dp', 'tp'), parts along dimension 0
- output 7: bfloat16 [10240, 9728], P('dp', 'tp'), parts along dimension 0
- output 8: bfloat16 [38912, 2560], P(('dp', 'tp')), parts along dimension 0
There are 4 independent parts. The reference program is written for one: setup_inputs(seed, part) draws one part's arguments, and reference() takes and returns one part's arrays. A program takes and returns all parts, laid end to end along the dimension named above; an argument that names none is the same for every part.
All inputs are finite; a program needn't handle non-finite values.
Results may differ from the reference program's by a relative error of at most 0.024.
Values are sent between devices in bfloat16 or wider.
A program may use at most 768 MiB of HBM per device.

```python
import jax
import jax.numpy as jnp
from jax import lax

SEQUENCES = 1
TOKENS = 2048
D = 2560
HEADS = 32
KV_HEADS = 8
HEAD = 128
FF = 9728
THETA = 10000
NAMES = ("wq", "wk", "wv", "wo", "w_gate", "w_up", "w_down")
SHAPES = {
    "wq": (D, HEADS * HEAD),
    "wk": (D, KV_HEADS * HEAD),
    "wv": (D, KV_HEADS * HEAD),
    "wo": (HEADS * HEAD, D),
    "w_gate": (D, FF),
    "w_up": (D, FF),
    "w_down": (FF, D),
}


def bump(key, n, height):
    away = (jnp.arange(n, dtype=jnp.int32) - jax.random.randint(key, (), 0, n, jnp.int32)) % n
    return jnp.where(away < n // 8, height, 1.0)


def together(key, own, strength):
    shared = jax.random.normal(key, own.shape[1:], jnp.float32)
    return (own + strength * shared) * lax.rsqrt(1 + strength * strength)


def setup_inputs(seed: int = 0, part: int = 0) -> dict:
    kx, kdy, ka, kb, kz, kf, kh, kl, *kw = jax.random.split(jax.random.key(seed), 8 + len(NAMES))
    kx, kdy, ka, kb = (jax.random.fold_in(k, part) for k in (kx, kdy, ka, kb))
    shape = (SEQUENCES, TOKENS, D)
    much_x, much_dy = jax.random.uniform(kz, (2,), jnp.float32, 0.0, 1.0)
    loud = 2.0 ** jax.random.uniform(jax.random.fold_in(kz, 1), (), jnp.float32, -1.0, 2.0)
    halves = 2.0 ** jax.random.uniform(kl, (2,), jnp.float32, -1.0, 1.0)
    times = {"wq": 1.0, "wk": 1.0, "wv": 2.0, "wo": halves[0], "w_gate": 1.0, "w_up": bump(kh, FF, 4.0), "w_down": halves[1]}
    x = together(ka, jax.random.normal(kx, shape, jnp.float32), much_x) * bump(kf, D, 4.0)
    dy = together(kb, jax.random.normal(kdy, shape, jnp.float32), much_dy)
    drawn = {"x": x.astype(jnp.bfloat16), "dy": (loud * dy * (SEQUENCES * TOKENS) ** -0.5).astype(jnp.bfloat16)}
    for key, name in zip(kw, NAMES, strict=True):
        drawn[name] = (jax.random.normal(key, SHAPES[name], jnp.float32) * SHAPES[name][0] ** -0.5 * times[name]).astype(jnp.bfloat16)
    return drawn


def matmul(a, w):
    return jnp.dot(a, w, preferred_element_type=jnp.float32).astype(jnp.bfloat16)


def normed(h):
    wide = h.astype(jnp.float32)
    scale = lax.rsqrt(jnp.mean(wide**2, -1, keepdims=True) + 1e-6)
    return (wide * scale).astype(jnp.bfloat16)


def turned(t, theta):
    half = t.shape[-1] // 2
    angle = jnp.arange(t.shape[0], dtype=jnp.float32)[:, None] * theta ** (-jnp.arange(half, dtype=jnp.float32) / half)
    cos, sin = jnp.cos(angle)[:, None], jnp.sin(angle)[:, None]
    a, b = t[..., :half].astype(jnp.float32), t[..., half:].astype(jnp.float32)
    return jnp.concatenate([a * cos - b * sin, b * cos + a * sin], -1).astype(jnp.bfloat16)


def seen_by(q, k, v):
    tokens, kv = q.shape[0], k.shape[1]
    q = q.reshape(tokens, kv, -1, q.shape[-1])
    scores = jnp.einsum("tgsd,ugd->gstu", q.astype(jnp.float32), k.astype(jnp.float32)) * q.shape[-1] ** -0.5
    place = jnp.arange(tokens)
    weights = jax.nn.softmax(jnp.where(place[:, None] >= place, scores, -jnp.inf), -1).astype(jnp.bfloat16)
    return jnp.einsum("gstu,ugd->tgsd", weights.astype(jnp.float32), v.astype(jnp.float32)).astype(jnp.bfloat16).reshape(tokens, -1)


def layer(h, w):
    a = normed(h)
    q, k = (turned(matmul(a, w[name]).reshape(h.shape[0], -1, HEAD), THETA) for name in ("wq", "wk"))
    h = h + matmul(seen_by(q, k, matmul(a, w["wv"]).reshape(h.shape[0], -1, HEAD)), w["wo"])
    b = normed(h)
    gate = jnp.dot(b, w["w_gate"], preferred_element_type=jnp.float32)
    up = jnp.dot(b, w["w_up"], preferred_element_type=jnp.float32)
    return h + matmul((jax.nn.silu(gate) * up).astype(jnp.bfloat16), w["w_down"])


def reference(x, dy, wq, wk, wv, wo, w_gate, w_up, w_down):
    weights = dict(zip(NAMES, (wq, wk, wv, wo, w_gate, w_up, w_down), strict=True))

    def take(so_far, sequence):
        h, by_y = sequence
        _, back = jax.vjp(lambda w, h: layer(h, w), weights, h)
        by_weights, by_h = back(by_y)
        return jax.tree.map(lambda total, term: total + term.astype(jnp.float32), so_far, by_weights), by_h

    none_yet = {name: jnp.zeros(w.shape, jnp.float32) for name, w in weights.items()}
    by_weights, by_x = lax.scan(take, none_yet, (x, dy))
    return (by_x, *(by_weights[name].astype(jnp.bfloat16) for name in NAMES))
```

```python
import functools

import jax
import jax.numpy as jnp
from jax import lax
from jax.experimental import pallas as pl
from jax.experimental.pallas import tpu as pltpu
from jax.sharding import PartitionSpec as P


HEAD = 128
THETA = 10000
NEG = -1e30
HIDDEN = 2 * NEG
LOG2E = 1.4426950408889634
VMEM = 56 * 2**20
BF = jnp.bfloat16
F32 = jnp.float32


def _dot(a, b, ca, cb):
    return lax.dot_general(a, b, (((ca,), (cb,)), ((), ())), preferred_element_type=F32)


def _turn(x, cos, sin, back=False):
    other = pltpu.roll(x, 64, 1) * sin
    return x * cos - other if back else x * cos + other


def _load_turned(refs, place_ref, cos_ref, sin_ref, to, heads):
    t = refs[0].shape[0]
    for c, ref in enumerate(refs):
        at = place_ref[c]
        rows = pl.ds(pl.multiple_of(at * t, t), t)
        cos, sin = cos_ref[rows, :], sin_ref[rows, :]
        for h in range(heads):
            lanes = slice(h * HEAD, (h + 1) * HEAD)
            to[at, :, lanes] = _turn(ref[:, lanes].astype(F32), cos, sin).astype(to.dtype)


def _attend_kernel(n, ids, heads, kv, place_ref, cos_ref, sin_ref, *refs):
    m = len(ids)
    take = iter(refs)
    some = lambda k: [next(take) for _ in range(k)]
    q_refs, k_refs, v_refs, o_refs, lse_refs = some(m), some(n), some(n), some(m), some(m)
    q_s, k_s, v_s, top_s, mix_s = some(5)
    t, g = q_refs[0].shape[0], heads // kv
    scale = HEAD**-0.5
    e = scale * LOG2E
    _load_turned(k_refs, place_ref, cos_ref, sin_ref, k_s, kv)
    for c in range(n):
        for i in range(kv):
            v_s[place_ref[c], i, :HEAD, :] = v_refs[c][:, i * HEAD : (i + 1) * HEAD].T
            v_s[place_ref[c], i, HEAD:, :] = jnp.ones((16, t), BF)

    def block(j, masked, k0=0, k1=t):
        scores = []
        for h in range(heads):
            i = h // g
            scores.append(_dot(k_s[j, k0:k1, i * HEAD : (i + 1) * HEAD], q_s[k0:, h * HEAD : (h + 1) * HEAD], 1, 1))
        if masked:
            ok = lax.broadcasted_iota(jnp.int32, (k1 - k0, t - k0), 1) >= lax.broadcasted_iota(jnp.int32, (k1 - k0, t - k0), 0)
        weights, keeps = [], []
        for h in range(heads):
            s = scores[h]
            if masked:
                s = jnp.where(ok, s, HIDDEN)
            old = top_s[h : h + 1, k0:]
            top = jnp.maximum(old, s.max(axis=0, keepdims=True))
            top_s[h : h + 1, k0:] = top
            weights.append(jnp.exp2((s - top) * e).astype(BF))
            keeps.append(jnp.exp2((old - top) * e))
        for h in range(heads):
            mix_s[h, :, k0:] = mix_s[h, :, k0:] * keeps[h] + _dot(v_s[j, h // g, :, k0:k1], weights[h], 1, 0)

    for x, c in enumerate(ids):
        iq = place_ref[c]
        rows = pl.ds(pl.multiple_of(iq * t, t), t)
        cos, sin = cos_ref[rows, :], sin_ref[rows, :]
        for h in range(heads):
            lanes = slice(h * HEAD, (h + 1) * HEAD)
            q_s[:, lanes] = _turn(q_refs[x][:, lanes].astype(F32), cos, sin).astype(BF)
        top_s[...] = jnp.full(top_s.shape, NEG, F32)
        mix_s[...] = jnp.zeros(mix_s.shape, F32)
        lax.fori_loop(0, iq, lambda j, _: block(j, False), None)
        block(iq, True, 0, t // 2)
        block(iq, True, t // 2, t)
        for h in range(heads):
            total = mix_s[h, HEAD : HEAD + 1, :]
            o_refs[x][:, h * HEAD : (h + 1) * HEAD] = (mix_s[h, :HEAD, :] * (1 / total)).T.astype(BF)
            lse_refs[x][h : h + 1, :] = top_s[h : h + 1, :] * scale + jnp.log(total)


def attend(ids, place, cos, sin, qs, ks, vs):
    n, m, (t, wide), few = len(ks), len(ids), qs[0].shape, ks[0].shape[1]
    heads, kv = wide // HEAD, few // HEAD
    vm = pl.BlockSpec(memory_space=pltpu.VMEM)
    got = pl.pallas_call(
        functools.partial(_attend_kernel, n, ids, heads, kv),
        in_specs=[pl.BlockSpec(memory_space=pltpu.SMEM)] + [vm] * (2 + m + 2 * n),
        out_specs=[vm] * (2 * m),
        out_shape=[jax.ShapeDtypeStruct((t, wide), BF)] * m + [jax.ShapeDtypeStruct((heads, t), F32)] * m,
        scratch_shapes=[pltpu.VMEM((t, wide), BF), pltpu.VMEM((n, t, few), BF), pltpu.VMEM((n, kv, HEAD + 16, t), BF),
                        pltpu.VMEM((heads, t), F32), pltpu.VMEM((heads, HEAD + 16, t), F32)],
        compiler_params=pltpu.CompilerParams(vmem_limit_bytes=VMEM),
        cost_estimate=pl.CostEstimate(flops=4 * heads * n * m * t * t * HEAD, transcendentals=heads * n * m * t * t // 2,
                                      bytes_accessed=m * t * wide * 5),
        name="attend",
    )(place, cos, sin, *qs, *ks, *vs)
    return got[:m], got[m:]


def _attend_bwd_kernel(n, ids, heads, kv, carried, final, place_ref, cos_ref, sin_ref, *refs):
    m = len(ids)
    take = iter(refs)
    some = lambda k: [next(take) for _ in range(k)]
    q_refs, k_refs, v_refs, do_refs, o_refs, lse_refs = some(m), some(n), some(n), some(m), some(m), some(m)
    so_far = some(2) if carried else None
    dq_refs = some(m)
    dk_refs, dv_refs = (some(n), some(n)) if final else (None, None)
    dk_s, dv_s, k_s, v_s, q_s, delta_s, dq_s = some(7)
    t, g = q_refs[0].shape[0], heads // kv
    scale = HEAD**-0.5
    e = scale * LOG2E
    _load_turned(k_refs, place_ref, cos_ref, sin_ref, k_s, kv)
    for c in range(n):
        v_s[place_ref[c]] = v_refs[c][...]
    if carried:
        dk_s[...], dv_s[...] = so_far[0][...], so_far[1][...]
    else:
        dk_s[...] = jnp.zeros(dk_s.shape, F32)
        dv_s[...] = jnp.zeros(dv_s.shape, F32)

    def block(do_ref, lse_ref, j, i, masked, k0=0, k1=t):
        lanes = slice(i * HEAD, (i + 1) * HEAD)
        k, v = k_s[j, k0:k1, lanes], v_s[j, k0:k1, lanes]
        kt = k.T
        if masked:
            ok = lax.broadcasted_iota(jnp.int32, (k1 - k0, t - k0), 1) >= lax.broadcasted_iota(jnp.int32, (k1 - k0, t - k0), 0)
        hs = range(i * g, (i + 1) * g)
        scores = [_dot(k, q_s[k0:, h * HEAD : (h + 1) * HEAD], 1, 1) for h in hs]
        dps = [_dot(v, do_ref[k0:, h * HEAD : (h + 1) * HEAD], 1, 1) for h in hs]
        by_v, by_k = dv_s[j, k0:k1, lanes], dk_s[j, k0:k1, lanes]
        for x, h in enumerate(hs):
            p = jnp.exp2(scores[x] * e - lse_ref[h : h + 1, k0:] * LOG2E)
            if masked:
                p = jnp.where(ok, p, 0.0)
            ds = (p * (dps[x] - delta_s[h : h + 1, k0:])).astype(BF)
            by_v += _dot(p.astype(BF), do_ref[k0:, h * HEAD : (h + 1) * HEAD], 1, 0)
            by_k += _dot(ds, q_s[k0:, h * HEAD : (h + 1) * HEAD], 1, 0)
            dq_s[h, :, k0:] += _dot(kt, ds, 1, 0)
        dv_s[j, k0:k1, lanes], dk_s[j, k0:k1, lanes] = by_v, by_k

    for x, c in enumerate(ids):
        iq, do_ref, lse_ref = place_ref[c], do_refs[x], lse_refs[x]
        rows = pl.ds(pl.multiple_of(iq * t, t), t)
        cos, sin = cos_ref[rows, :], sin_ref[rows, :]
        for h in range(heads):
            lanes = slice(h * HEAD, (h + 1) * HEAD)
            q_s[:, lanes] = _turn(q_refs[x][:, lanes].astype(F32), cos, sin).astype(BF)
            both = do_ref[:, lanes].astype(F32) * o_refs[x][:, lanes].astype(F32)
            delta_s[h : h + 1, :] = both.T.sum(axis=0, keepdims=True)
        dq_s[...] = jnp.zeros(dq_s.shape, F32)
        for i in range(kv):
            lax.fori_loop(0, iq, lambda j, _: block(do_ref, lse_ref, j, i, False), None)
            block(do_ref, lse_ref, iq, i, True, 0, t // 2)
            block(do_ref, lse_ref, iq, i, True, t // 2, t)
        for h in range(heads):
            dq = (dq_s[h] * scale).T.astype(BF).astype(F32)
            dq_refs[x][:, h * HEAD : (h + 1) * HEAD] = _turn(dq, cos, sin, True).astype(BF)

    if final:
        for c in range(n):
            j = place_ref[c]
            rows = pl.ds(pl.multiple_of(j * t, t), t)
            cos, sin = cos_ref[rows, :], sin_ref[rows, :]
            for i in range(kv):
                lanes = slice(i * HEAD, (i + 1) * HEAD)
                dk = (dk_s[j, :, lanes] * scale).astype(BF).astype(F32)
                dk_refs[c][:, lanes] = _turn(dk, cos, sin, True).astype(BF)
            dv_refs[c][...] = dv_s[j].astype(BF)


def attend_bwd(ids, place, cos, sin, qs, ks, vs, dos, outs, lses, so_far=None, final=False):
    n, (t, wide), few, m = len(ks), qs[0].shape, ks[0].shape[1], len(ids)
    heads, kv = wide // HEAD, few // HEAD
    vm = pl.BlockSpec(memory_space=pltpu.VMEM)
    carried = so_far is not None
    sums = [jax.ShapeDtypeStruct((n, t, few), F32)] * 2
    held = [pltpu.VMEM((n, t, few), F32)] * 2
    rest = [jax.ShapeDtypeStruct((t, few), BF)] * (2 * n) if final else sums
    given = [*qs, *ks, *vs, *dos, *outs, *lses, *(so_far or ())]
    got = pl.pallas_call(
        functools.partial(_attend_bwd_kernel, n, ids, heads, kv, carried, final),
        in_specs=[pl.BlockSpec(memory_space=pltpu.SMEM)] + [vm] * (2 + len(given)),
        out_specs=[vm] * (m + len(rest)),
        out_shape=[jax.ShapeDtypeStruct((t, wide), BF)] * m + rest,
        scratch_shapes=(held if final else []) + [pltpu.VMEM((n, t, few), BF), pltpu.VMEM((n, t, few), BF), pltpu.VMEM((t, wide), BF),
                                                  pltpu.VMEM((heads, t), F32), pltpu.VMEM((heads, HEAD, t), F32)],
        compiler_params=pltpu.CompilerParams(vmem_limit_bytes=VMEM),
        cost_estimate=pl.CostEstimate(flops=8 * m * heads * n * t * t * HEAD, transcendentals=m * heads * n * t * t // 2,
                                      bytes_accessed=m * t * wide * 9),
        name="attend_bwd",
    )(place, cos, sin, *given)
    return (got[:m], got[m : m + n], got[m + n :]) if final else (got[:m], (got[m], got[m + 1]))


def weight_grads(a, bs, rows=512, only=None, into=None):
    n, (t, m) = len(a), a[0].shape
    widths = [b[0].shape[1] for b in bs]
    flat = [p for b in bs for p in b]
    first, end = only or (0, pl.cdiv(m, rows))

    def kernel(*refs):
        a_refs, b_refs, outs = refs[:n], refs[n : n + len(flat)], refs[-len(bs) :]
        for o, out in enumerate(outs):
            total = None
            for c in range(n):
                d = _dot(a_refs[c][...], b_refs[o * n + c][...], 0, 0)
                total = d if total is None else total + d
            out[...] = total.astype(out.dtype)

    given = [*a, *flat] + ([] if into is None else [into])
    return pl.pallas_call(
        kernel,
        grid=(end - first,),
        in_specs=[pl.BlockSpec((t, rows), lambda i: (0, i + first)) for _ in a] + [pl.BlockSpec(p.shape, lambda i: (0, 0)) for p in flat]
        + ([] if into is None else [pl.BlockSpec(memory_space=pl.ANY)]),
        out_specs=[pl.BlockSpec((rows, w), lambda i: (i + first, 0)) for w in widths],
        out_shape=[jax.ShapeDtypeStruct((m, w), BF) for w in widths],
        input_output_aliases={} if into is None else {len(given) - 1: 0},
        compiler_params=pltpu.CompilerParams(dimension_semantics=("arbitrary",), vmem_limit_bytes=VMEM),
        cost_estimate=pl.CostEstimate(flops=2 * n * t * min((end - first) * rows, m) * sum(widths), transcendentals=0,
                                      bytes_accessed=2 * (n * t + m) * (m + sum(widths))),
    )(*given)


def mmt_sum(many, ws, tile, halves=False):
    t, m, p = many[0][0].shape[0], ws[0].shape[0], len(ws)
    k = [w.shape[1] for w in ws]
    given = [a for one in many for a in one]
    cut = 2 if halves else 1

    def kernel(*refs):
        for c in range(len(many)):
            total = None
            for a, w in zip(refs[c * p : (c + 1) * p], refs[len(given) : len(given) + p]):
                d = _dot(a[...], w[...], 1, 1)
                total = d if total is None else total + d
            outs = refs[len(given) + p + c * cut : len(given) + p + (c + 1) * cut]
            for r, out in enumerate(outs):
                out[...] = total[r * (t // cut) : (r + 1) * (t // cut), :].astype(BF)

    return pl.pallas_call(
        kernel,
        grid=(pl.cdiv(m, tile),),
        in_specs=[pl.BlockSpec(a.shape, lambda i: (0, 0)) for a in given] + [pl.BlockSpec((tile, d), lambda i: (i, 0)) for d in k],
        out_specs=[pl.BlockSpec((t // cut, tile), lambda i: (0, i))] * (cut * len(many)),
        out_shape=[jax.ShapeDtypeStruct((t // cut, m), BF)] * (cut * len(many)),
        compiler_params=pltpu.CompilerParams(dimension_semantics=("arbitrary",), vmem_limit_bytes=VMEM),
        cost_estimate=pl.CostEstimate(flops=2 * len(many) * t * m * sum(k), transcendentals=0,
                                      bytes_accessed=2 * (len(many) * t * (m + sum(k)) + m * sum(k))),
    )(*given, *ws)


def mm_each(many, ws, steps):
    t, k = many[0].shape
    m = [w.shape[1] for w in ws]

    def kernel(*refs):
        outs = iter(refs[len(many) + len(ws) :])
        for a in refs[: len(many)]:
            for w in refs[len(many) : len(many) + len(ws)]:
                next(outs)[...] = _dot(a[...], w[...], 1, 0).astype(BF)

    got = pl.pallas_call(
        kernel,
        grid=(steps,),
        in_specs=[pl.BlockSpec((t, k), lambda i: (0, 0)) for _ in many] + [pl.BlockSpec((k, d // steps), lambda i: (0, i)) for d in m],
        out_specs=[pl.BlockSpec((t, d // steps), lambda i: (0, i)) for d in m] * len(many),
        out_shape=[jax.ShapeDtypeStruct((t, d), BF) for d in m] * len(many),
        compiler_params=pltpu.CompilerParams(dimension_semantics=("arbitrary",), vmem_limit_bytes=VMEM),
        cost_estimate=pl.CostEstimate(flops=2 * len(many) * t * k * sum(m), transcendentals=0,
                                      bytes_accessed=2 * (len(many) * t * (k + sum(m)) + k * sum(m))),
    )(*many, *ws)
    return [got[c * len(ws) : (c + 1) * len(ws)] for c in range(len(many))]


def mlp(b, by_hidden, wg, wu, tile=512, parts=2, halves=False):
    (t, d), f = b.shape, wg.shape[1]
    steps = pl.cdiv(f, tile)
    last = f - (steps - 1) * tile
    cut_in = 2 if halves else 1

    def kernel(b_ref, d_ref, g_ref, u_ref, h_ref, dg_ref, du_ref, *rest):
        db_refs, sum_s = rest[:-1], rest[-1]
        at = pl.program_id(0)

        def part(w, first):
            for r in range(0, t, t // parts):
                rows = slice(r, r + t // parts)
                x = b_ref[rows, :]
                gate, up, by = _dot(x, g_ref[:, :w], 1, 0), _dot(x, u_ref[:, :w], 1, 0), d_ref[rows, :w].astype(F32)
                s = jax.nn.sigmoid(gate)
                silu = gate * s
                h_ref[rows, :w] = (silu * up).astype(BF)
                dg, du = (by * up * (s + silu * (1 - s))).astype(BF), (by * silu).astype(BF)
                dg_ref[rows, :w], du_ref[rows, :w] = dg, du
                db = _dot(dg, g_ref[:, :w], 1, 1) + _dot(du, u_ref[:, :w], 1, 1)
                if first:
                    sum_s[rows, :] = db
                else:
                    sum_s[rows, :] += db

        pl.when(at == 0)(lambda: part(tile, True))
        pl.when((at > 0) & (at < steps - 1))(lambda: part(tile, False))

        @pl.when(at == steps - 1)
        def _():
            part(last, False)
            for r, db_ref in enumerate(db_refs):
                db_ref[...] = sum_s[r * (t // cut_in) : (r + 1) * (t // cut_in), :].astype(BF)

    whole, cut = pl.BlockSpec((t, d), lambda i: (0, 0)), pl.BlockSpec((t, tile), lambda i: (0, i))
    weight = pl.BlockSpec((d, tile), lambda i: (0, i))
    return pl.pallas_call(
        kernel,
        grid=(steps,),
        in_specs=[whole, cut, weight, weight],
        out_specs=[cut, cut, cut] + [pl.BlockSpec((t // cut_in, d), lambda i: (0, 0))] * cut_in,
        out_shape=[jax.ShapeDtypeStruct((t, f), BF)] * 3 + [jax.ShapeDtypeStruct((t // cut_in, d), BF)] * cut_in,
        scratch_shapes=[pltpu.VMEM((t, d), F32)],
        compiler_params=pltpu.CompilerParams(dimension_semantics=("arbitrary",), vmem_limit_bytes=VMEM),
        cost_estimate=pl.CostEstimate(flops=8 * t * d * f, transcendentals=t * f, bytes_accessed=4 * t * d + 8 * t * f + 4 * d * f),
    )(b, by_hidden, wg, wu)


def shift(x, n, by):
    return lax.ppermute(x, "tp", [(i, (i + by) % n) for i in range(n)])


def gather_near(h, n):
    return shift(h, n, 1), shift(h, n, -1)


def gather_far(left, right, n):
    half = left.shape[0] // 2
    return jnp.concatenate([shift(left[:half], n, 1), shift(right[half:], n, -1)])


def rowwise(f, given, outs, rows=128, starts=None, aliases=None):
    t, d = given[0].shape
    steps = t // rows if starts is None else min(a.shape[0] for a in given) // rows
    starts = starts or [0] * (len(given) + outs)
    shapes = [(t, d)] * outs

    def kernel(*refs):
        for ref, value in zip(refs[len(given) :], f(*[r[...].astype(F32) for r in refs[: len(given)]])):
            ref[...] = value.astype(BF)

    specs = [pl.BlockSpec((rows, d), lambda i, at=at: (i + at, 0)) for at in starts]
    return pl.pallas_call(
        kernel,
        grid=(steps,),
        in_specs=specs[: len(given)],
        out_specs=specs[len(given) :],
        out_shape=[jax.ShapeDtypeStruct(shape, BF) for shape in shapes],
        input_output_aliases=aliases or {},
        compiler_params=pltpu.CompilerParams(dimension_semantics=("arbitrary",), vmem_limit_bytes=32 * 2**20),
        cost_estimate=pl.CostEstimate(flops=8 * steps * rows * d, transcendentals=0, bytes_accessed=2 * steps * rows * d * (len(given) + outs)),
    )(*given)


def scatter(own, left, right, far, n):
    from_left, from_right = shift(far[0], n, 1), shift(far[1], n, -1)
    at = left.shape[0] // 2 // 64
    right, left = rowwise(lambda a, b, x, y: (a + x, b + y), [right, left, from_left, from_right], 2, 64,
                          [0, at, 0, 0, 0, at], {0: 0, 1: 1})
    return own, shift(right, n, 1), shift(left, n, -1)


def rounded(x):
    return x.astype(BF).astype(F32)


def scale_of(wide):
    return lax.rsqrt(jnp.mean(wide**2, -1, keepdims=True) + 1e-6)


def normed(h):
    return rowwise(lambda wide: (wide * scale_of(wide),), [h], 1)[0]


def added_and_normed(x, terms):
    def f(x, a, b, c):
        h = rounded(x + rounded(a + b + c))
        return h, h * scale_of(h)

    return rowwise(f, [x, *terms], 2)


def norm_bwd(h, rest, terms):
    def f(wide, rest, a, b, c):
        by, scale = rounded(a + b + c), scale_of(wide)
        return (rest + rounded(by * scale - wide * (scale**3 * jnp.mean(by * wide, -1, keepdims=True))),)

    return rowwise(f, [h, rest, *terms], 1)[0]


def mm(a, w):
    return _dot(a, w, 1, 0).astype(BF)


def step(n, x, dy, wq, wk, wv, wo, wg, wu, wd):
    t = x.shape[0]
    me = lax.axis_index("tp")
    place = jnp.stack([me, (me + n - 1) % n, (me + 1) % n, (me + 2) % n]).astype(jnp.int32)
    half = HEAD // 2
    angle = jnp.arange(n * t, dtype=F32)[:, None] * THETA ** (-jnp.arange(half, dtype=F32) / half)
    cos, sin = jnp.cos(angle), jnp.sin(angle)
    cos, sin = jnp.concatenate([cos, cos], 1), jnp.concatenate([-sin, sin], 1)

    def gathered(h):
        left, right = gather_near(h, n)
        return [h, left, right, gather_far(left, right, n)]

    a = gathered(normed(x))
    qkv = [*mm_each(a[:1], (wq, wk, wv), 2), *mm_each(a[1:3], (wq, wk, wv), 2), *mm_each(a[3:], (wq, wk, wv), 2)]
    qs, ks, vs = ([z[m] for z in qkv] for m in range(3))
    dys = gathered(dy)
    (out_far,), (lse_far,) = attend((3,), place, cos, sin, qs[3:], ks, vs)
    outs, lses = attend((0, 1, 2), place, cos, sin, qs[:3], ks, vs)
    outs, lses = [*outs, out_far], [*lses, lse_far]
    attended = scatter(*[mm(outs[c], wo) for c in range(3)], (mm(out_far[: t // 2], wo), mm(out_far[t // 2 :], wo)), n)
    by_hidden = [*mmt_sum([[c] for c in dys[:3]], [wd], 512), *mmt_sum([[dys[3]]], [wd], 512)]
    h, normed_h = added_and_normed(x, attended)

    b = gathered(normed_h)
    done = []
    for c in range(4):
        done.append(mlp(b[c], by_hidden[c], wg, wu, halves=c == 3))
    hidden, by_gate, by_up = ([z[m] for z in done] for m in range(3))
    by_h = norm_bwd(h, dy, scatter(*[z[3] for z in done[:3]], done[3][3:], n))

    (g_wd,) = weight_grads(hidden, [dys])
    (g_wg,) = weight_grads(b, [by_gate])
    (g_wu,) = weight_grads(b, [by_up], only=(0, 3))
    (g_wu,) = weight_grads(b, [by_up], only=(3, pl.cdiv(b[0].shape[1], 512)), into=g_wu)

    dhs = gathered(by_h)
    by_out = [*mmt_sum([[dhs[0]]], [wo], 512), *mmt_sum([[dhs[1]], [dhs[2]]], [wo], 512),
              *mmt_sum([[dhs[3]]], [wo], 512)]

    def back(ids, so_far, final=False):
        return attend_bwd(ids, place, cos, sin, [qs[c] for c in ids], ks, vs, [by_out[c] for c in ids], [outs[c] for c in ids], [lses[c] for c in ids], so_far, final)

    dq_near, so_far = back((0, 1, 2), None)
    dq_far, dks, dvs = back((3,), so_far, True)
    each = list(zip([*dq_near, *dq_far], dks, dvs))
    by_a = [*mmt_sum(each[:1], [wq, wk, wv], 640), *mmt_sum(each[1:3], [wq, wk, wv], 640),
            mmt_sum(each[3:], [wq, wk, wv], 640, True)]
    by_x = norm_bwd(x, by_h, scatter(*by_a, n))
    (g_wo,) = weight_grads(outs, [dhs])
    g_wq, g_wk, g_wv = weight_grads(a, list(zip(*each)))
    return by_x, g_wq, g_wk, g_wv, g_wo, g_wg, g_wu, g_wd


def solution(mesh):
    n = mesh.shape["tp"]

    def run(x, dy, *weights):
        by_x, *grads = step(n, x[0], dy[0], *weights)
        return (by_x[None], *grads)

    states, by_columns, by_rows = P("dp", "tp", None), P(None, "tp"), P("tp", None)
    weights = (by_columns, by_columns, by_columns, by_rows, by_columns, by_columns, by_rows)
    own = tuple(P("dp", "tp") if spec == by_columns else P(("dp", "tp"), None) for spec in weights)
    return jax.shard_map(run, mesh=mesh, in_specs=(states, states, *weights), out_specs=(states, *own), check_vma=False)
```

```python
import functools

import jax
import jax.numpy as jnp
from jax import lax
from jax.experimental import pallas as pl
from jax.experimental.pallas import tpu as pltpu
from jax.sharding import PartitionSpec as P


HEAD = 128
THETA = 10000
PIECE = 256
NEG = -1e30
HIDDEN = 2 * NEG
LOG2E = 1.4426950408889634
VMEM = 56 * 2**20
BF = jnp.bfloat16
F32 = jnp.float32


def _dot(a, b, ca, cb):
    return lax.dot_general(a, b, (((ca,), (cb,)), ((), ())), preferred_element_type=F32)


def _turn(x, cos, sin, back=False):
    other = pltpu.roll(x, 64, 1) * sin
    return x * cos - other if back else x * cos + other


def _load_turned(refs, place_ref, cos_ref, sin_ref, to, heads):
    t = refs[0].shape[0]
    for c, ref in enumerate(refs):
        at = place_ref[c]
        rows = pl.ds(pl.multiple_of(at * t, t), t)
        cos, sin = cos_ref[rows, :], sin_ref[rows, :]
        for h in range(heads):
            lanes = slice(h * HEAD, (h + 1) * HEAD)
            to[at, :, lanes] = _turn(ref[:, lanes].astype(F32), cos, sin).astype(to.dtype)


def _attend_kernel(n, ids, heads, kv, place_ref, cos_ref, sin_ref, *refs):
    m = len(ids)
    take = iter(refs)
    some = lambda k: [next(take) for _ in range(k)]
    q_refs, k_refs, v_refs, o_refs, lse_refs = some(m), some(n), some(n), some(m), some(m)
    q_s, k_s, v_s, top_s, mix_s = some(5)
    t, g = q_refs[0].shape[0], heads // kv
    scale = HEAD**-0.5
    e = scale * LOG2E
    _load_turned(k_refs, place_ref, cos_ref, sin_ref, k_s, kv)
    for c in range(n):
        for i in range(kv):
            v_s[place_ref[c], i, :HEAD, :] = v_refs[c][:, i * HEAD : (i + 1) * HEAD].T
            v_s[place_ref[c], i, HEAD:, :] = jnp.ones((16, t), BF)

    def block(j, masked, k0=0, k1=t):
        scores = []
        for h in range(heads):
            i = h // g
            scores.append(_dot(k_s[j, k0:k1, i * HEAD : (i + 1) * HEAD], q_s[k0:, h * HEAD : (h + 1) * HEAD], 1, 1))
        if masked:
            ok = lax.broadcasted_iota(jnp.int32, (k1 - k0, t - k0), 1) >= lax.broadcasted_iota(jnp.int32, (k1 - k0, t - k0), 0)
        weights, keeps = [], []
        for h in range(heads):
            s = scores[h]
            if masked:
                s = jnp.where(ok, s, HIDDEN)
            old = top_s[h : h + 1, k0:]
            top = jnp.maximum(old, s.max(axis=0, keepdims=True))
            top_s[h : h + 1, k0:] = top
            weights.append(jnp.exp2((s - top) * e).astype(BF))
            keeps.append(jnp.exp2((old - top) * e))
        for h in range(heads):
            mix_s[h, :, k0:] = mix_s[h, :, k0:] * keeps[h] + _dot(v_s[j, h // g, :, k0:k1], weights[h], 1, 0)

    for x, c in enumerate(ids):
        iq = place_ref[c]
        rows = pl.ds(pl.multiple_of(iq * t, t), t)
        cos, sin = cos_ref[rows, :], sin_ref[rows, :]
        for h in range(heads):
            lanes = slice(h * HEAD, (h + 1) * HEAD)
            q_s[:, lanes] = _turn(q_refs[x][:, lanes].astype(F32), cos, sin).astype(BF)
        top_s[...] = jnp.full(top_s.shape, NEG, F32)
        mix_s[...] = jnp.zeros(mix_s.shape, F32)
        lax.fori_loop(0, iq, lambda j, _: block(j, False), None)
        block(iq, True, 0, t // 2)
        block(iq, True, t // 2, t)
        for h in range(heads):
            total = mix_s[h, HEAD : HEAD + 1, :]
            o_refs[x][:, h * HEAD : (h + 1) * HEAD] = (mix_s[h, :HEAD, :] * (1 / total)).T.astype(BF)
            lse_refs[x][h : h + 1, :] = top_s[h : h + 1, :] * scale + jnp.log(total)


def attend(ids, place, cos, sin, qs, ks, vs):
    n, m, (t, wide), few = len(ks), len(ids), qs[0].shape, ks[0].shape[1]
    heads, kv = wide // HEAD, few // HEAD
    vm = pl.BlockSpec(memory_space=pltpu.VMEM)
    got = pl.pallas_call(
        functools.partial(_attend_kernel, n, ids, heads, kv),
        in_specs=[pl.BlockSpec(memory_space=pltpu.SMEM)] + [vm] * (2 + m + 2 * n),
        out_specs=[vm] * (2 * m),
        out_shape=[jax.ShapeDtypeStruct((t, wide), BF)] * m + [jax.ShapeDtypeStruct((heads, t), F32)] * m,
        scratch_shapes=[pltpu.VMEM((t, wide), BF), pltpu.VMEM((n, t, few), BF), pltpu.VMEM((n, kv, HEAD + 16, t), BF),
                        pltpu.VMEM((heads, t), F32), pltpu.VMEM((heads, HEAD + 16, t), F32)],
        compiler_params=pltpu.CompilerParams(vmem_limit_bytes=VMEM),
        cost_estimate=pl.CostEstimate(flops=4 * heads * n * m * t * t * HEAD, transcendentals=heads * n * m * t * t // 2,
                                      bytes_accessed=m * t * wide * 5),
        name="attend",
    )(place, cos, sin, *qs, *ks, *vs)
    return got[:m], got[m:]


def _attend_bwd_kernel(n, ids, heads, kv, carried, final, place_ref, cos_ref, sin_ref, *refs):
    m = len(ids)
    take = iter(refs)
    some = lambda k: [next(take) for _ in range(k)]
    q_refs, k_refs, v_refs, do_refs, o_refs, lse_refs = some(m), some(n), some(n), some(m), some(m), some(m)
    so_far = some(2) if carried else None
    dq_refs = some(m)
    dk_refs, dv_refs = (some(n), some(n)) if final else (None, None)
    dk_s, dv_s, k_s, v_s, q_s, delta_s, dq_s = some(7)
    t, g = q_refs[0].shape[0], heads // kv
    scale = HEAD**-0.5
    e = scale * LOG2E
    _load_turned(k_refs, place_ref, cos_ref, sin_ref, k_s, kv)
    for c in range(n):
        v_s[place_ref[c]] = v_refs[c][...]
    if carried:
        dk_s[...], dv_s[...] = so_far[0][...], so_far[1][...]
    else:
        dk_s[...] = jnp.zeros(dk_s.shape, F32)
        dv_s[...] = jnp.zeros(dv_s.shape, F32)

    def block(do_ref, lse_ref, j, i, masked, k0=0, k1=t):
        lanes = slice(i * HEAD, (i + 1) * HEAD)
        k, v = k_s[j, k0:k1, lanes], v_s[j, k0:k1, lanes]
        kt = k.T
        if masked:
            ok = lax.broadcasted_iota(jnp.int32, (k1 - k0, t - k0), 1) >= lax.broadcasted_iota(jnp.int32, (k1 - k0, t - k0), 0)
        hs = range(i * g, (i + 1) * g)
        scores = [_dot(k, q_s[k0:, h * HEAD : (h + 1) * HEAD], 1, 1) for h in hs]
        dps = [_dot(v, do_ref[k0:, h * HEAD : (h + 1) * HEAD], 1, 1) for h in hs]
        by_v, by_k = dv_s[j, k0:k1, lanes], dk_s[j, k0:k1, lanes]
        for x, h in enumerate(hs):
            p = jnp.exp2(scores[x] * e - lse_ref[h : h + 1, k0:] * LOG2E)
            if masked:
                p = jnp.where(ok, p, 0.0)
            ds = (p * (dps[x] - delta_s[h : h + 1, k0:])).astype(BF)
            by_v += _dot(p.astype(BF), do_ref[k0:, h * HEAD : (h + 1) * HEAD], 1, 0)
            by_k += _dot(ds, q_s[k0:, h * HEAD : (h + 1) * HEAD], 1, 0)
            dq_s[h, :, k0:] += _dot(kt, ds, 1, 0)
        dv_s[j, k0:k1, lanes], dk_s[j, k0:k1, lanes] = by_v, by_k

    for x, c in enumerate(ids):
        iq, do_ref, lse_ref = place_ref[c], do_refs[x], lse_refs[x]
        rows = pl.ds(pl.multiple_of(iq * t, t), t)
        cos, sin = cos_ref[rows, :], sin_ref[rows, :]
        for h in range(heads):
            lanes = slice(h * HEAD, (h + 1) * HEAD)
            q_s[:, lanes] = _turn(q_refs[x][:, lanes].astype(F32), cos, sin).astype(BF)
            both = do_ref[:, lanes].astype(F32) * o_refs[x][:, lanes].astype(F32)
            delta_s[h : h + 1, :] = both.T.sum(axis=0, keepdims=True)
        dq_s[...] = jnp.zeros(dq_s.shape, F32)
        for i in range(kv):
            lax.fori_loop(0, iq, lambda j, _: block(do_ref, lse_ref, j, i, False), None)
            block(do_ref, lse_ref, iq, i, True, 0, t // 2)
            block(do_ref, lse_ref, iq, i, True, t // 2, t)
        for h in range(heads):
            dq = (dq_s[h] * scale).T.astype(BF).astype(F32)
            dq_refs[x][:, h * HEAD : (h + 1) * HEAD] = _turn(dq, cos, sin, True).astype(BF)

    if final:
        for c in range(n):
            j = place_ref[c]
            rows = pl.ds(pl.multiple_of(j * t, t), t)
            cos, sin = cos_ref[rows, :], sin_ref[rows, :]
            for i in range(kv):
                lanes = slice(i * HEAD, (i + 1) * HEAD)
                dk = (dk_s[j, :, lanes] * scale).astype(BF).astype(F32)
                dk_refs[c][:, lanes] = _turn(dk, cos, sin, True).astype(BF)
            dv_refs[c][...] = dv_s[j].astype(BF)


def attend_bwd(ids, place, cos, sin, qs, ks, vs, dos, outs, lses, so_far=None, final=False):
    n, (t, wide), few, m = len(ks), qs[0].shape, ks[0].shape[1], len(ids)
    heads, kv = wide // HEAD, few // HEAD
    vm = pl.BlockSpec(memory_space=pltpu.VMEM)
    carried = so_far is not None
    sums = [jax.ShapeDtypeStruct((n, t, few), F32)] * 2
    held = [pltpu.VMEM((n, t, few), F32)] * 2
    rest = [jax.ShapeDtypeStruct((t, few), BF)] * (2 * n) if final else sums
    given = [*qs, *ks, *vs, *dos, *outs, *lses, *(so_far or ())]
    got = pl.pallas_call(
        functools.partial(_attend_bwd_kernel, n, ids, heads, kv, carried, final),
        in_specs=[pl.BlockSpec(memory_space=pltpu.SMEM)] + [vm] * (2 + len(given)),
        out_specs=[vm] * (m + len(rest)),
        out_shape=[jax.ShapeDtypeStruct((t, wide), BF)] * m + rest,
        scratch_shapes=(held if final else []) + [pltpu.VMEM((n, t, few), BF), pltpu.VMEM((n, t, few), BF), pltpu.VMEM((t, wide), BF),
                                                  pltpu.VMEM((heads, t), F32), pltpu.VMEM((heads, HEAD, t), F32)],
        compiler_params=pltpu.CompilerParams(vmem_limit_bytes=VMEM),
        cost_estimate=pl.CostEstimate(flops=8 * m * heads * n * t * t * HEAD, transcendentals=m * heads * n * t * t // 2,
                                      bytes_accessed=m * t * wide * 9),
        name="attend_bwd",
    )(place, cos, sin, *given)
    return (got[:m], got[m : m + n], got[m + n :]) if final else (got[:m], (got[m], got[m + 1]))


def weight_grads(a, bs, rows=512, only=None, into=None):
    n, m, t = len(a), a[0][0].shape[1], PIECE
    widths = [b[0][0].shape[1] for b in bs]
    flat = [p for b in bs for p in b]
    first, end = only or (0, pl.cdiv(m, rows))

    def kernel(*refs):
        outs = refs[-len(bs) :]
        x = jnp.concatenate([r[...] for r in refs[:n]])
        for o, out in enumerate(outs):
            out[...] = _dot(x, jnp.concatenate([r[...] for r in refs[(o + 1) * n : (o + 2) * n]]), 0, 0).astype(out.dtype)

    given = [p[0] for p in (*a, *flat)] + ([] if into is None else [into])
    return pl.pallas_call(
        kernel,
        grid=(end - first,),
        in_specs=[pl.BlockSpec((t, rows), lambda i, r=r: (r, i + first)) for _, r in a]
        + [pl.BlockSpec((t, p.shape[1]), lambda i, r=r: (r, 0)) for p, r in flat]
        + ([] if into is None else [pl.BlockSpec(memory_space=pl.ANY)]),
        out_specs=[pl.BlockSpec((rows, w), lambda i: (i + first, 0)) for w in widths],
        out_shape=[jax.ShapeDtypeStruct((m, w), BF) for w in widths],
        input_output_aliases={} if into is None else {len(given) - 1: 0},
        compiler_params=pltpu.CompilerParams(dimension_semantics=("arbitrary",), vmem_limit_bytes=VMEM),
        cost_estimate=pl.CostEstimate(flops=2 * n * t * min((end - first) * rows, m) * sum(widths), transcendentals=0,
                                      bytes_accessed=2 * (n * t + m) * (m + sum(widths))),
    )(*given)


def mmt_sum(many, ws, tile, halves=False):
    t, m, p = many[0][0].shape[0], ws[0].shape[0], len(ws)
    k = [w.shape[1] for w in ws]
    given = [a for one in many for a in one]
    cut = 2 if halves else 1

    def kernel(*refs):
        for c in range(len(many)):
            total = None
            for a, w in zip(refs[c * p : (c + 1) * p], refs[len(given) : len(given) + p]):
                d = _dot(a[...], w[...], 1, 1)
                total = d if total is None else total + d
            outs = refs[len(given) + p + c * cut : len(given) + p + (c + 1) * cut]
            for r, out in enumerate(outs):
                out[...] = total[r * (t // cut) : (r + 1) * (t // cut), :].astype(BF)

    return pl.pallas_call(
        kernel,
        grid=(pl.cdiv(m, tile),),
        in_specs=[pl.BlockSpec(a.shape, lambda i: (0, 0)) for a in given] + [pl.BlockSpec((tile, d), lambda i: (i, 0)) for d in k],
        out_specs=[pl.BlockSpec((t // cut, tile), lambda i: (0, i))] * (cut * len(many)),
        out_shape=[jax.ShapeDtypeStruct((t // cut, m), BF)] * (cut * len(many)),
        compiler_params=pltpu.CompilerParams(dimension_semantics=("arbitrary",), vmem_limit_bytes=VMEM),
        cost_estimate=pl.CostEstimate(flops=2 * len(many) * t * m * sum(k), transcendentals=0,
                                      bytes_accessed=2 * (len(many) * t * (m + sum(k)) + m * sum(k))),
    )(*given, *ws)


def mm_each(many, ws, steps):
    t, k = many[0].shape
    m = [w.shape[1] for w in ws]

    def kernel(*refs):
        outs = iter(refs[len(many) + len(ws) :])
        for a in refs[: len(many)]:
            for w in refs[len(many) : len(many) + len(ws)]:
                next(outs)[...] = _dot(a[...], w[...], 1, 0).astype(BF)

    got = pl.pallas_call(
        kernel,
        grid=(steps,),
        in_specs=[pl.BlockSpec((t, k), lambda i: (0, 0)) for _ in many] + [pl.BlockSpec((k, d // steps), lambda i: (0, i)) for d in m],
        out_specs=[pl.BlockSpec((t, d // steps), lambda i: (0, i)) for d in m] * len(many),
        out_shape=[jax.ShapeDtypeStruct((t, d), BF) for d in m] * len(many),
        compiler_params=pltpu.CompilerParams(dimension_semantics=("arbitrary",), vmem_limit_bytes=VMEM),
        cost_estimate=pl.CostEstimate(flops=2 * len(many) * t * k * sum(m), transcendentals=0,
                                      bytes_accessed=2 * (len(many) * t * (k + sum(m)) + k * sum(m))),
    )(*many, *ws)
    return [got[c * len(ws) : (c + 1) * len(ws)] for c in range(len(many))]


def mlp(b, by_hidden, wg, wu, tile=512, halves=True):
    d, f = wg.shape
    t, parts = len(b) * PIECE, len(b)
    steps = pl.cdiv(f, tile)
    last = f - (steps - 1) * tile
    cut_in = 2 if halves else 1

    def kernel(*refs):
        b_refs, d_refs, (g_ref, u_ref, h_ref, dg_ref, du_ref) = refs[:parts], refs[parts : 2 * parts], refs[2 * parts : 2 * parts + 5]
        db_refs, sum_s = refs[2 * parts + 5 : -1], refs[-1]
        at = pl.program_id(0)

        def part(w, first):
            for b_ref, d_ref, r in zip(b_refs, d_refs, range(0, t, PIECE)):
                rows = slice(r, r + PIECE)
                x = b_ref[...]
                gate, up, by = _dot(x, g_ref[:, :w], 1, 0), _dot(x, u_ref[:, :w], 1, 0), d_ref[:, :w].astype(F32)
                s = jax.nn.sigmoid(gate)
                silu = gate * s
                h_ref[rows, :w] = (silu * up).astype(BF)
                dg, du = (by * up * (s + silu * (1 - s))).astype(BF), (by * silu).astype(BF)
                dg_ref[rows, :w], du_ref[rows, :w] = dg, du
                db = _dot(dg, g_ref[:, :w], 1, 1) + _dot(du, u_ref[:, :w], 1, 1)
                if first:
                    sum_s[rows, :] = db
                else:
                    sum_s[rows, :] += db

        pl.when(at == 0)(lambda: part(tile, True))
        pl.when((at > 0) & (at < steps - 1))(lambda: part(tile, False))

        @pl.when(at == steps - 1)
        def _():
            part(last, False)
            for r, db_ref in enumerate(db_refs):
                db_ref[...] = sum_s[r * (t // cut_in) : (r + 1) * (t // cut_in), :].astype(BF)

    cut = pl.BlockSpec((t, tile), lambda i: (0, i))
    weight = pl.BlockSpec((d, tile), lambda i: (0, i))
    return pl.pallas_call(
        kernel,
        grid=(steps,),
        in_specs=[pl.BlockSpec((PIECE, d), lambda i, r=r: (r, 0)) for _, r in b]
        + [pl.BlockSpec((PIECE, tile), lambda i, r=r: (r, i)) for _, r in by_hidden]
        + [weight, weight],
        out_specs=[cut, cut, cut] + [pl.BlockSpec((t // cut_in, d), lambda i: (0, 0))] * cut_in,
        out_shape=[jax.ShapeDtypeStruct((t, f), BF)] * 3 + [jax.ShapeDtypeStruct((t // cut_in, d), BF)] * cut_in,
        scratch_shapes=[pltpu.VMEM((t, d), F32)],
        compiler_params=pltpu.CompilerParams(dimension_semantics=("arbitrary",), vmem_limit_bytes=VMEM),
        cost_estimate=pl.CostEstimate(flops=8 * t * d * f, transcendentals=t * f, bytes_accessed=4 * t * d + 8 * t * f + 4 * d * f),
    )(*[p[0] for p in b], *[p[0] for p in by_hidden], wg, wu)


def shift(x, n, by):
    return lax.ppermute(x, "tp", [(i, (i + by) % n) for i in range(n)])


def gather_near(h, n):
    return shift(h, n, 1), shift(h, n, -1)


def gather_far(left, right, n):
    half = left.shape[0] // 2
    return jnp.concatenate([shift(left[:half], n, 1), shift(right[half:], n, -1)])


def rowwise(f, given, outs, rows=128):
    given = [a if isinstance(a, tuple) else (a,) for a in given]
    t, d = sum(a.shape[0] for a in given[0]), given[0][0].shape[1]
    half = t // 2 // rows
    at = {(1, 0): lambda i: (i, 0), (2, 0): lambda i: (jnp.minimum(i, half - 1), 0), (2, 1): lambda i: (jnp.maximum(i - half, 0), 0)}
    counts = [len(a) for a in given] + [2 if pair else 1 for pair in outs]
    specs = [pl.BlockSpec((rows, d), at[k, m]) for k in counts for m in range(k)]
    flat = [x for a in given for x in a]

    def kernel(*refs):
        take = iter(refs)
        refs = [[next(take) for _ in range(k)] for k in counts]

        def part(m):
            mine = [r[m if len(r) == 2 else 0] for r in refs]
            for ref, value in zip(mine[len(given) :], f(*[r[...].astype(F32) for r in mine[: len(given)]])):
                ref[...] = value.astype(BF)

        for m in range(2):
            pl.when((pl.program_id(0) >= half) == (m == 1))(functools.partial(part, m))

    got = pl.pallas_call(
        kernel,
        grid=(2 * half,),
        in_specs=specs[: len(flat)],
        out_specs=specs[len(flat) :],
        out_shape=[jax.ShapeDtypeStruct((t // 2, d) if pair else (t, d), BF) for pair in outs for _ in range(2 if pair else 1)],
        compiler_params=pltpu.CompilerParams(dimension_semantics=("arbitrary",), vmem_limit_bytes=32 * 2**20),
        cost_estimate=pl.CostEstimate(flops=8 * t * d, transcendentals=0, bytes_accessed=2 * t * d * (len(given) + len(outs))),
    )(*flat)
    take = iter(got)
    return [(next(take), next(take)) if pair else next(take) for pair in outs]


def joined(left, right, from_left, from_right, at):
    rows, d = 64, left.shape[1]

    def kernel(r_ref, l_ref, x_ref, y_ref, r_out, l_out):
        r_out[...] = (r_ref[...].astype(F32) + x_ref[...].astype(F32)).astype(BF)
        l_out[...] = (l_ref[...].astype(F32) + y_ref[...].astype(F32)).astype(BF)

    here = pl.BlockSpec((rows, d), lambda i: (i, 0))
    there = pl.BlockSpec((rows, d), lambda i: (i + at, 0))
    right, left = pl.pallas_call(
        kernel,
        grid=(from_left.shape[0] // rows,),
        in_specs=[here, there, here, here],
        out_specs=[here, there],
        out_shape=[jax.ShapeDtypeStruct(right.shape, BF), jax.ShapeDtypeStruct(left.shape, BF)],
        input_output_aliases={0: 0, 1: 1},
        compiler_params=pltpu.CompilerParams(dimension_semantics=("arbitrary",), vmem_limit_bytes=32 * 2**20),
        cost_estimate=pl.CostEstimate(flops=4 * from_left.size, transcendentals=0, bytes_accessed=12 * from_left.size),
    )(right, left, from_left, from_right)
    return left, right


def scatter(own, left, right, far, n):
    from_left, from_right = shift(far[0], n, 1), shift(far[1], n, -1)
    left, right = joined(left, right, from_left, from_right, left.shape[0] // 2 // 64)
    return own, shift(right, n, 1), shift(left, n, -1)


def rounded(x):
    return x.astype(BF).astype(F32)


def scale_of(wide):
    return lax.rsqrt(jnp.mean(wide**2, -1, keepdims=True) + 1e-6)


def normed(h):
    return rowwise(lambda wide: (wide * scale_of(wide),), [h], [False])[0]


def added_and_normed(x, terms):
    def f(x, a, b, c):
        h = rounded(x + rounded(a + b + c))
        return h, h * scale_of(h)

    return rowwise(f, [x, *terms], [False, True])


def norm_bwd(h, rest, terms):
    def f(wide, rest, a, b, c):
        by, scale = rounded(a + b + c), scale_of(wide)
        return (rest + rounded(by * scale - wide * (scale**3 * jnp.mean(by * wide, -1, keepdims=True))),)

    return rowwise(f, [h, rest, *terms], [False])[0]


def pieces(chunks):
    return [(x, r) for x in chunks for r in range(2)]


def mm(a, w):
    return _dot(a, w, 1, 0).astype(BF)


def step(n, x, dy, wq, wk, wv, wo, wg, wu, wd):
    t = x.shape[0]
    me = lax.axis_index("tp")
    place = jnp.stack([me, (me + n - 1) % n, (me + 1) % n, (me + 2) % n]).astype(jnp.int32)
    half = HEAD // 2
    angle = jnp.arange(n * t, dtype=F32)[:, None] * THETA ** (-jnp.arange(half, dtype=F32) / half)
    cos, sin = jnp.cos(angle), jnp.sin(angle)
    cos, sin = jnp.concatenate([cos, cos], 1), jnp.concatenate([-sin, sin], 1)

    def gathered(h):
        left, right = gather_near(h, n)
        return [h, left, right, gather_far(left, right, n)]

    a = gathered(normed(x))
    qkv = [*mm_each(a[:1], (wq, wk, wv), 2), *mm_each(a[1:3], (wq, wk, wv), 2), *mm_each(a[3:], (wq, wk, wv), 2)]
    qs, ks, vs = ([z[m] for z in qkv] for m in range(3))
    dys = gathered(dy)
    (out_far,), (lse_far,) = attend((3,), place, cos, sin, qs[3:], ks, vs)
    outs, lses = attend((0, 1, 2), place, cos, sin, qs[:3], ks, vs)
    outs, lses = [*outs, out_far], [*lses, lse_far]
    attended = scatter(*[mm(outs[c], wo) for c in range(3)], (mm(out_far[: t // 2], wo), mm(out_far[t // 2 :], wo)), n)
    by_hidden = [*mmt_sum([[c] for c in dys[:3]], [wd], 512), *mmt_sum([[dys[3]]], [wd], 512)]
    h, normed_h = added_and_normed(x, attended)

    left = [shift(normed_h[0], n, 1), shift(normed_h[1], n, 1)]
    right = [shift(normed_h[0], n, -1), shift(normed_h[1], n, -1)]
    far = [shift(left[0], n, 1), shift(right[1], n, -1)]
    whole = lambda x: [(x, 0), (x, 1)]
    mixed = lambda z: [*whole(z[0]), (z[1], 0), (z[2], 0), (z[1], 1), (z[2], 1), *whole(z[3])]
    b = [(x, 0) for x in (*normed_h, left[0], right[0], left[1], right[1], *far)]
    by_hidden = mixed(by_hidden)
    done = []
    for c in range(4):
        done.append(mlp(b[2 * c : 2 * c + 2], by_hidden[2 * c : 2 * c + 2], wg, wu, halves=c > 0))
    hidden, by_gate, by_up = ([p for z in done for p in whole(z[m])] for m in range(3))
    (left_a, right_a), (left_b, right_b), (far_a, far_b) = (z[3:] for z in done[1:])
    by_left_b, by_right_a = shift(right_b, n, 1), shift(left_a, n, -1)
    left_b, right_a = joined(left_b, right_a, shift(far_a, n, 1), shift(far_b, n, -1), 0)
    by_left_a, by_right_b = shift(right_a, n, 1), shift(left_b, n, -1)
    by_h = norm_bwd(h, dy, (done[0][3], (by_left_a, by_left_b), (by_right_a, by_right_b)))

    (g_wd,) = weight_grads(hidden, [mixed(dys)])
    (g_wg,) = weight_grads(b, [by_gate])
    (g_wu,) = weight_grads(b, [by_up], only=(0, 3))
    (g_wu,) = weight_grads(b, [by_up], only=(3, pl.cdiv(wg.shape[0], 512)), into=g_wu)

    dhs = gathered(by_h)
    by_out = [*mmt_sum([[dhs[0]]], [wo], 512), *mmt_sum([[dhs[1]], [dhs[2]]], [wo], 512),
              *mmt_sum([[dhs[3]]], [wo], 512)]

    def back(ids, so_far, final=False):
        return attend_bwd(ids, place, cos, sin, [qs[c] for c in ids], ks, vs, [by_out[c] for c in ids], [outs[c] for c in ids], [lses[c] for c in ids], so_far, final)

    dq_near, so_far = back((0, 1, 2), None)
    dq_far, dks, dvs = back((3,), so_far, True)
    each = list(zip([*dq_near, *dq_far], dks, dvs))
    by_a = [*mmt_sum(each[:1], [wq, wk, wv], 640), *mmt_sum(each[1:3], [wq, wk, wv], 640),
            mmt_sum(each[3:], [wq, wk, wv], 640, True)]
    by_x = norm_bwd(x, by_h, scatter(*by_a, n))
    (g_wo,) = weight_grads(pieces(outs), [pieces(dhs)])
    g_wq, g_wk, g_wv = weight_grads(pieces(a), [pieces(z) for z in zip(*each)])
    return by_x, g_wq, g_wk, g_wv, g_wo, g_wg, g_wu, g_wd


def solution(mesh):
    n = mesh.shape["tp"]

    def run(x, dy, *weights):
        by_x, *grads = step(n, x[0], dy[0], *weights)
        return (by_x[None], *grads)

    states, by_columns, by_rows = P("dp", "tp", None), P(None, "tp"), P("tp", None)
    weights = (by_columns, by_columns, by_columns, by_rows, by_columns, by_columns, by_rows)
    own = tuple(P("dp", "tp") if spec == by_columns else P(("dp", "tp"), None) for spec in weights)
    return jax.shard_map(run, mesh=mesh, in_specs=(states, states, *weights), out_specs=(states, *own), check_vma=False)
```
